8 devices in a mesh: dp: 2 (over z, y), sp: 4 (over x, core).
Axes of the slice: x: 2, y: 2, z: 1, core: 2. Of those that a mesh axis runs over, the one named last changes fastest.
Arguments:
- hidden: bfloat16 [16, 1536, 3072], P('dp', 'sp'), parts along dimension 0
- cond_vec: bfloat16 [16, 3072], P('dp'), parts along dimension 0
- pos_ids: int32 [1536, 3], P('sp')
- w_mod: bfloat16 [2, 3072, 9216], replicated
- b_mod: bfloat16 [2, 9216], replicated
- w_in: bfloat16 [2, 3072, 21504], replicated
- b_in: bfloat16 [2, 21504], replicated
- q_gain: bfloat16 [2, 128], replicated
- k_gain: bfloat16 [2, 128], replicated
- w_out: bfloat16 [2, 15360, 3072], replicated
- b_out: bfloat16 [2, 3072], replicated
Outputs:
- output: bfloat16 [16, 1536, 3072], P('dp', 'sp'), parts along dimension 0
There are 2 independent parts. The reference program is written for one: setup_inputs(seed, part) draws one part's arguments, and reference() takes and returns one part's arrays. A program takes and returns all parts, laid end to end along the dimension named above; an argument that names none is the same for every part.
All inputs are finite; a program needn't handle non-finite values.
Results may differ from the reference program's by a relative error of at most 0.0114649.
Values are sent between devices in bfloat16 or wider.
A program may use at most 2.5 GiB of HBM per device.

```python
import math
import jax
import jax.numpy as jnp
from jax import lax

BATCH = 8
TEXT_LEN = 512
IMG_LEN = 1024
D = 3072
HEADS = 24
HEAD = 128
MLP_DIM = 12288
BLOCKS = 2
QUERY_ROWS = 256

SEQ_LEN = TEXT_LEN + IMG_LEN
ROPE_SPLIT = (16, 56, 56)
ROPE_THETA = 10000.0
NORM_EPS = 1e-6


def image_ids(rng_key):
    half_log = int(math.log2(IMG_LEN)) // 2
    widths = jnp.array([2 ** (half_log - 1), 2 ** half_log, 2 ** (half_log + 1)], dtype=jnp.int32)
    k_width, k_row, k_col = jax.random.split(rng_key, 3)
    grid_width = widths[jax.random.randint(k_width, (), 0, 3)]
    row_off = jax.random.randint(k_row, (), 0, 64)
    col_off = jax.random.randint(k_col, (), 0, 64)
    img_index = jnp.arange(IMG_LEN, dtype=jnp.int32)
    img_ids = jnp.stack([jnp.zeros_like(img_index), row_off + img_index // grid_width, col_off + img_index % grid_width], axis=1)
    return jnp.concatenate([jnp.zeros((TEXT_LEN, 3), jnp.int32), img_ids.astype(jnp.int32)], axis=0)


def setup_inputs(seed: int = 0, part: int = 0) -> dict:
    shared = jax.random.split(jax.random.key(seed), 9)
    part_key = jax.random.fold_in(jax.random.key(seed + 1), part)
    k_text, k_img, k_mean, k_cond = jax.random.split(part_key, 4)
    text_mean = jax.random.normal(k_mean, (D,), jnp.float32)
    text_rows = 0.6 * jax.random.normal(k_text, (BATCH, TEXT_LEN, D), jnp.float32) + text_mean
    img_rows = jax.random.normal(k_img, (BATCH, IMG_LEN, D), jnp.float32)
    hidden = jnp.concatenate([text_rows, img_rows], axis=1).astype(jnp.bfloat16)
    cond_vec = jax.random.normal(k_cond, (BATCH, D), jnp.float32).astype(jnp.bfloat16)
    pos_ids = image_ids(shared[0])
    w_mod = (jax.random.normal(shared[1], (BLOCKS, D, 3 * D), jnp.float32) * D ** -0.5).astype(jnp.bfloat16)
    b_mod = (0.3 * jax.random.normal(shared[2], (BLOCKS, 3 * D), jnp.float32)).astype(jnp.bfloat16)
    w_in = (jax.random.normal(shared[3], (BLOCKS, D, 3 * D + MLP_DIM), jnp.float32) * D ** -0.5).astype(jnp.bfloat16)
    b_in = (0.3 * jax.random.normal(shared[4], (BLOCKS, 3 * D + MLP_DIM), jnp.float32)).astype(jnp.bfloat16)
    q_gain = jax.random.uniform(shared[5], (BLOCKS, HEAD), jnp.float32, 0.8, 2.2).astype(jnp.bfloat16)
    k_gain = jax.random.uniform(shared[6], (BLOCKS, HEAD), jnp.float32, 0.8, 2.2).astype(jnp.bfloat16)
    w_out = (jax.random.normal(shared[7], (BLOCKS, D + MLP_DIM, D), jnp.float32) * (D + MLP_DIM) ** -0.5).astype(jnp.bfloat16)
    b_out = (0.3 * jax.random.normal(shared[8], (BLOCKS, D), jnp.float32)).astype(jnp.bfloat16)
    return dict(hidden=hidden, cond_vec=cond_vec, pos_ids=pos_ids, w_mod=w_mod, b_mod=b_mod, w_in=w_in, b_in=b_in, q_gain=q_gain, k_gain=k_gain, w_out=w_out, b_out=b_out)


def rope_tables(pos_ids):
    angle_parts = []
    for column, rope_dim in enumerate(ROPE_SPLIT):
        inv_freq = 1.0 / (ROPE_THETA ** (jnp.arange(0, rope_dim, 2, dtype=jnp.float32) / rope_dim))
        angle_parts.append(pos_ids[:, column:column + 1].astype(jnp.float32) * inv_freq)
    angles = jnp.concatenate(angle_parts, axis=1)
    return jnp.cos(angles), jnp.sin(angles)


def rms_norm(tensor, gain):
    sq_mean = jnp.mean(tensor * tensor, axis=-1, keepdims=True)
    return tensor * lax.rsqrt(sq_mean + NORM_EPS) * gain.astype(jnp.float32)


def apply_rope(tensor, cos_t, sin_t):
    paired = tensor.reshape(tensor.shape[:-1] + (tensor.shape[-1] // 2, 2))
    even_v = paired[..., 0]
    odd_v = paired[..., 1]
    cos_b = cos_t[:, None, :]
    sin_b = sin_t[:, None, :]
    rotated = jnp.stack([even_v * cos_b - odd_v * sin_b, even_v * sin_b + odd_v * cos_b], axis=-1)
    return rotated.reshape(tensor.shape)


def attention(queries, keys_all, values_all):
    key_f = keys_all.astype(jnp.float32)
    val_f = values_all.astype(jnp.float32)
    q_blocks = queries.reshape(SEQ_LEN // QUERY_ROWS, QUERY_ROWS, HEADS, HEAD)

    def one_block(q_blk):
        scores = jnp.einsum('qhd,khd->hqk', q_blk.astype(jnp.float32), key_f) * HEAD ** -0.5
        probs = jax.nn.softmax(scores, axis=-1)
        return jnp.einsum('hqk,khd->qhd', probs, val_f)

    return lax.map(one_block, q_blocks).reshape(SEQ_LEN, HEADS, HEAD).astype(jnp.bfloat16)


def single_block(hidden, cond_row, cos_t, sin_t, params):
    w_mod, b_mod, w_in, b_in, q_gain, k_gain, w_out, b_out = params
    mod_act = jax.nn.silu(cond_row.astype(jnp.float32)).astype(jnp.bfloat16)
    mod_vals = jnp.dot(mod_act[None, :], w_mod, preferred_element_type=jnp.float32)[0] + b_mod.astype(jnp.float32)
    mod_vals = mod_vals.astype(jnp.bfloat16).astype(jnp.float32)
    mod_shift = mod_vals[:D]
    mod_scale = mod_vals[D:2 * D]
    mod_gate = mod_vals[2 * D:]
    x_float = hidden.astype(jnp.float32)
    centered = x_float - jnp.mean(x_float, axis=-1, keepdims=True)
    normed = centered * lax.rsqrt(jnp.mean(centered * centered, axis=-1, keepdims=True) + NORM_EPS)
    modded = ((1.0 + mod_scale) * normed + mod_shift).astype(jnp.bfloat16)
    proj_in = (jnp.dot(modded, w_in, preferred_element_type=jnp.float32) + b_in.astype(jnp.float32)).astype(jnp.bfloat16)
    q_raw = proj_in[:, :D].reshape(SEQ_LEN, HEADS, HEAD).astype(jnp.float32)
    k_raw = proj_in[:, D:2 * D].reshape(SEQ_LEN, HEADS, HEAD).astype(jnp.float32)
    v_heads = proj_in[:, 2 * D:3 * D].reshape(SEQ_LEN, HEADS, HEAD)
    q_heads = apply_rope(rms_norm(q_raw, q_gain), cos_t, sin_t).astype(jnp.bfloat16)
    k_heads = apply_rope(rms_norm(k_raw, k_gain), cos_t, sin_t).astype(jnp.bfloat16)
    attn_out = attention(q_heads, k_heads, v_heads).reshape(SEQ_LEN, D)
    mlp_act = jax.nn.gelu(proj_in[:, 3 * D:].astype(jnp.float32), approximate=True).astype(jnp.bfloat16)
    joined = jnp.concatenate([attn_out, mlp_act], axis=1)
    block_out = (jnp.dot(joined, w_out, preferred_element_type=jnp.float32) + b_out.astype(jnp.float32)).astype(jnp.bfloat16)
    return (x_float + mod_gate * block_out.astype(jnp.float32)).astype(jnp.bfloat16)


def reference(hidden, cond_vec, pos_ids, w_mod, b_mod, w_in, b_in, q_gain, k_gain, w_out, b_out):
    cos_t, sin_t = rope_tables(pos_ids)
    stacked = (w_mod, b_mod, w_in, b_in, q_gain, k_gain, w_out, b_out)

    def one_item(item_pair):
        tokens, cond_row = item_pair

        def layer_step(state, params):
            return single_block(state, cond_row, cos_t, sin_t, params), None

        final_x, _ = lax.scan(layer_step, tokens, stacked)
        return final_x

    return lax.map(one_item, (hidden, cond_vec))
```

```python
import functools
import math
import jax
import jax.numpy as jnp
from jax import lax
from jax.experimental import pallas as pl
from jax.experimental.pallas import tpu as pltpu
from jax.sharding import PartitionSpec as P

HEAD = 128
ROPE_SPLIT = (16, 56, 56)
ROPE_THETA = 10000.0
NORM_EPS = 1e-6
MIB = 1024 * 1024
LN_ROWS = 16


def rope_tables(pos):
    parts = []
    for column, rope_dim in enumerate(ROPE_SPLIT):
        inv_freq = 1.0 / (ROPE_THETA ** (jnp.arange(0, rope_dim, 2, dtype=jnp.float32) / rope_dim))
        parts.append(pos[..., column:column + 1].astype(jnp.float32) * jnp.repeat(inv_freq, 2))
    angles = jnp.concatenate(parts, axis=-1)
    sign = jnp.where(jnp.arange(HEAD) % 2 == 0, -1.0, 1.0)
    return jnp.cos(angles), jnp.sin(angles) * sign


def mod_kernel(me_ref, c_ref, w_ref, b_ref, o_ref):
    act = jax.nn.silu(c_ref[...].astype(jnp.float32)).astype(jnp.bfloat16)
    vals = jnp.dot(act, w_ref[0], preferred_element_type=jnp.float32) + b_ref[0].astype(jnp.float32)
    o_ref[0] = vals.astype(jnp.bfloat16)


def modulation(cond_vec, w_mod, b_mod, me, n_shard):
    n_layer, dim, width = w_mod.shape
    n_item = cond_vec.shape[0]
    share = width // n_shard
    cols = share // 2
    return pl.pallas_call(
        mod_kernel,
        grid_spec=pltpu.PrefetchScalarGridSpec(
            num_scalar_prefetch=1,
            grid=(n_layer, 2),
            in_specs=[
                pl.BlockSpec((n_item, dim), lambda l, j, me: (0, 0)),
                pl.BlockSpec((1, dim, cols), lambda l, j, me: (l, 0, me[0] * 2 + j)),
                pl.BlockSpec((1, 1, cols), lambda l, j, me: (l, 0, me[0] * 2 + j)),
            ],
            out_specs=pl.BlockSpec((1, n_item, cols), lambda l, j, me: (l, 0, j)),
        ),
        out_shape=jax.ShapeDtypeStruct((n_layer, n_item, share), jnp.bfloat16),
        compiler_params=pltpu.CompilerParams(vmem_limit_bytes=48 * MIB),
        name="modulation",
    )(me, cond_vec, w_mod, b_mod)


def proj_in_kernel(x_ref, mod_ref, w_ref, b_ref, gain_ref, cos_ref, sin_ref, *rest, n_qk, n_v, sub, cols):
    out_ref, u_ref, acc_ref = rest[-3:]
    j = pl.program_id(1)
    _, n_item, rows, dim = x_ref.shape
    width = w_ref.shape[2]

    @pl.when(j == 0)
    def _():
        for t in range(n_item):
            shift = mod_ref[t, :, :dim]
            scale = 1.0 + mod_ref[t, :, dim:2 * dim]

            def norm_step(i, carry):
                r = pl.ds(pl.multiple_of(i * LN_ROWS, LN_ROWS), LN_ROWS)
                x = x_ref[0, t, r, :].astype(jnp.float32)
                x = x - jnp.mean(x, axis=-1, keepdims=True)
                x = x * lax.rsqrt(jnp.mean(x * x, axis=-1, keepdims=True) + NORM_EPS)
                u_ref[t, r, :] = (scale * x + shift).astype(jnp.bfloat16)
                return carry

            lax.fori_loop(0, rows // LN_ROWS, norm_step, 0)

    def pieces(finish):
        waiting = None
        slot = 0
        for t in range(n_item):
            for s in range(rows // sub):
                for n in range(width // cols):
                    r = slice(s * sub, (s + 1) * sub)
                    acc_ref[slot] = jnp.dot(u_ref[t, r, :], w_ref[0, :, n * cols:(n + 1) * cols], preferred_element_type=jnp.float32)
                    if waiting is not None:
                        finish(*waiting)
                    waiting = (slot, t, r, n * cols)
                    slot = 1 - slot
        finish(*waiting)

    def biased(slot, c0):
        return (acc_ref[slot] + b_ref[0, :, c0:c0 + cols].astype(jnp.float32)).astype(jnp.bfloat16)

    @pl.when(j < 2 * n_qk)
    def _():
        gain = jnp.where(j < n_qk, gain_ref[0], gain_ref[1])
        even = lax.broadcasted_iota(jnp.int32, (sub, HEAD), 1) % 2 == 0

        def finish(slot, t, r, c0):
            h = biased(slot, c0).astype(jnp.float32)
            for d in range(0, cols, HEAD):
                v = h[:, d:d + HEAD]
                v = v * lax.rsqrt(jnp.mean(v * v, axis=-1, keepdims=True) + NORM_EPS) * gain
                swapped = jnp.where(even, pltpu.roll(v, HEAD - 1, 1), pltpu.roll(v, 1, 1))
                out_ref[0, t, r, c0 + d:c0 + d + HEAD] = (v * cos_ref[0, r, :] + swapped * sin_ref[0, r, :]).astype(jnp.bfloat16)

        pieces(finish)

    @pl.when((j >= 2 * n_qk) & (j < 2 * n_qk + n_v))
    def _():
        def finish(slot, t, r, c0):
            out_ref[0, t, r, c0:c0 + cols] = biased(slot, c0)

        pieces(finish)

    @pl.when(j >= 2 * n_qk + n_v)
    def _():
        def finish(slot, t, r, c0):
            h = biased(slot, c0).astype(jnp.float32)
            out_ref[0, t, r, c0:c0 + cols] = jax.nn.gelu(h, approximate=True).astype(jnp.bfloat16)

        pieces(finish)


def proj_in(x, mod, w_in, b_in, gain, cos, sin, layer, n_chunk, first=0, prev=None, block=1536, sub=192, cols=512):
    count, n_item, rows, dim = x.shape
    width = w_in.shape[2]
    in_specs = [
        pl.BlockSpec((1, n_item, rows, dim), lambda r, j: (r, 0, 0, 0)),
        pl.BlockSpec((n_item, 1, 3 * dim), lambda r, j: (0, 0, 0)),
        pl.BlockSpec((1, dim, block), lambda r, j: (layer, 0, j)),
        pl.BlockSpec((1, 1, block), lambda r, j: (layer, 0, j)),
        pl.BlockSpec((2, 1, HEAD), lambda r, j: (0, 0, 0)),
        pl.BlockSpec((1, rows, HEAD), lambda r, j: (first + r, 0, 0)),
        pl.BlockSpec((1, rows, HEAD), lambda r, j: (first + r, 0, 0)),
    ]
    operands = [x, mod, w_in, b_in, gain, cos, sin]
    aliases = {}
    if prev is not None:
        in_specs.append(pl.BlockSpec(memory_space=pl.ANY))
        operands.append(prev)
        aliases = {7: 0}
    return pl.pallas_call(
        functools.partial(proj_in_kernel, n_qk=dim // block, n_v=dim // block, sub=sub, cols=cols),
        grid=(count, width // block),
        in_specs=in_specs,
        out_specs=pl.BlockSpec((1, n_item, rows, block), lambda r, j: (first + r, 0, 0, j)),
        out_shape=jax.ShapeDtypeStruct((n_chunk, n_item, rows, width), jnp.bfloat16),
        scratch_shapes=[pltpu.VMEM((n_item, rows, dim), jnp.bfloat16), pltpu.VMEM((2, sub, cols), jnp.float32)],
        input_output_aliases=aliases,
        compiler_params=pltpu.CompilerParams(vmem_limit_bytes=60 * MIB),
        cost_estimate=pl.CostEstimate(flops=2 * count * n_item * rows * dim * width, bytes_accessed=2 * count * (dim * width + n_item * rows * width), transcendentals=0),
        name="proj_in",
    )(*operands)


def attention_kernel(q_ref, k_ref, v_ref, o_ref, s_ref, *, n_head, sub):
    n_chunk, _, rows, _ = q_ref.shape
    keys = n_chunk * rows
    exp_scale = HEAD ** -0.5 * math.log2(math.e)
    work = [(slice(h * HEAD, (h + 1) * HEAD), c, slice(s * sub, (s + 1) * sub)) for h in range(n_head) for c in range(n_chunk) for s in range(rows // sub)]

    def score(i):
        head, c, r = work[i]
        k = k_ref[:, 0, :, head].reshape(keys, HEAD)
        s_ref[i % 2] = lax.dot_general(q_ref[c, 0, r, head], k, (((1,), (1,)), ((), ())), preferred_element_type=jnp.float32)

    score(0)
    for i, (head, c, r) in enumerate(work):
        if i + 1 < len(work):
            score(i + 1)
        s = s_ref[i % 2]
        p = jnp.exp2((s - jnp.max(s, axis=-1, keepdims=True)) * exp_scale)
        total = jnp.sum(p, axis=-1, keepdims=True)
        v = v_ref[:, 0, :, head].reshape(keys, HEAD)
        o = jnp.dot(p.astype(jnp.bfloat16), v, preferred_element_type=jnp.float32)
        o_ref[c, 0, r, head] = (o / total).astype(jnp.bfloat16)


def attention(h, dim, n_head=4, sub=384):
    n_chunk, n_item, rows, _ = h.shape
    w = n_head * HEAD
    nb = dim // w
    block = (n_chunk, 1, rows, w)
    keys = n_chunk * rows
    return pl.pallas_call(
        functools.partial(attention_kernel, n_head=n_head, sub=sub),
        grid=(n_item, nb),
        in_specs=[
            pl.BlockSpec(block, lambda t, g: (0, t, 0, g)),
            pl.BlockSpec(block, lambda t, g: (0, t, 0, nb + g)),
            pl.BlockSpec(block, lambda t, g: (0, t, 0, 2 * nb + g)),
        ],
        out_specs=pl.BlockSpec(block, lambda t, g: (0, t, 0, g)),
        out_shape=jax.ShapeDtypeStruct((n_chunk, n_item, rows, dim), jnp.bfloat16),
        scratch_shapes=[pltpu.VMEM((2, sub, keys), jnp.float32)],
        compiler_params=pltpu.CompilerParams(vmem_limit_bytes=60 * MIB),
        cost_estimate=pl.CostEstimate(flops=4 * n_item * keys * keys * dim, bytes_accessed=8 * n_item * keys * dim, transcendentals=n_item * keys * keys * dim // HEAD),
        name="attention",
    )(h, h, h)


def proj_out_kernel(slot_ref, o_ref, g_ref, w_ref, b_ref, x_ref, mod_ref, *rest, k_attn, sub, cols):
    out_ref, acc_ref = rest[-2:]
    k = pl.program_id(1)
    last = pl.num_programs(1) - 1
    n_item, rows, dim = acc_ref.shape
    tiles = [(t, slice(s * sub, (s + 1) * sub), slice(n * cols, (n + 1) * cols)) for t in range(n_item) for s in range(rows // sub) for n in range(dim // cols)]

    def product(src, t, r, c):
        return jnp.dot(src[0, t, r, :], w_ref[0, :, c], preferred_element_type=jnp.float32)

    @pl.when(k == 0)
    def _():
        for t, r, c in tiles:
            acc_ref[t, r, c] = product(o_ref, t, r, c)

    @pl.when((k > 0) & (k < k_attn))
    def _():
        for t, r, c in tiles:
            acc_ref[t, r, c] += product(o_ref, t, r, c)

    @pl.when((k >= k_attn) & (k < last))
    def _():
        for t, r, c in tiles:
            acc_ref[t, r, c] += product(g_ref, t, r, c)

    @pl.when(k == last)
    def _():
        for t, r, c in tiles:
            y = acc_ref[t, r, c] + product(g_ref, t, r, c) + b_ref[0, :, c].astype(jnp.float32)
            gate = mod_ref[t, :, 2 * dim + c.start:2 * dim + c.stop]
            y = gate * y.astype(jnp.bfloat16).astype(jnp.float32)
            out_ref[0, t, r, c] = (x_ref[0, t, r, c].astype(jnp.float32) + y).astype(jnp.bfloat16)


def proj_out(o, h, w_out, b_out, x, mod, layer, slot, out_slots, first=0, x_first=0, count=None, prev=None, k_block=1536, sub=384, cols=512):
    n_chunk, n_item, rows, dim = o.shape
    depth = w_out.shape[1]
    k_attn = dim // k_block
    g_off = 3 * dim // k_block - k_attn
    in_specs = [
        pl.BlockSpec((1, n_item, rows, k_block), lambda r, k, sl: (first + r, 0, 0, jnp.minimum(k, k_attn - 1))),
        pl.BlockSpec((1, n_item, rows, k_block), lambda r, k, sl: (first + r, 0, 0, g_off + jnp.maximum(k, k_attn))),
        pl.BlockSpec((1, k_block, dim), lambda r, k, sl: (layer, k, 0)),
        pl.BlockSpec((1, 1, dim), lambda r, k, sl: (layer, 0, 0)),
        pl.BlockSpec((1, n_item, rows, dim), lambda r, k, sl: (x_first + r, 0, 0, 0)),
        pl.BlockSpec((n_item, 1, 3 * dim), lambda r, k, sl: (0, 0, 0)),
    ]
    operands = [slot, o, h, w_out, b_out, x, mod]
    aliases = {}
    if prev is not None:
        in_specs.append(pl.BlockSpec(memory_space=pl.ANY))
        operands.append(prev)
        aliases = {7: 0}
    return pl.pallas_call(
        functools.partial(proj_out_kernel, k_attn=k_attn, sub=sub, cols=cols),
        grid_spec=pltpu.PrefetchScalarGridSpec(
            num_scalar_prefetch=1,
            grid=(count, depth // k_block),
            in_specs=in_specs,
            out_specs=pl.BlockSpec((1, n_item, rows, dim), lambda r, k, sl: (sl[0] + r, 0, 0, 0)),
            scratch_shapes=[pltpu.VMEM((n_item, rows, dim), jnp.float32)],
        ),
        out_shape=jax.ShapeDtypeStruct((out_slots, n_item, rows, dim), jnp.bfloat16),
        input_output_aliases=aliases,
        compiler_params=pltpu.CompilerParams(vmem_limit_bytes=62 * MIB),
        cost_estimate=pl.CostEstimate(flops=2 * count * n_item * rows * dim * depth, bytes_accessed=2 * count * dim * depth, transcendentals=0),
        name="proj_out",
    )(*operands)


def solution(mesh):
    row_spec = P('dp', 'sp', None)
    n_shard = mesh.shape['sp']

    def local_forward(hidden, cond_vec, pos_ids, w_mod, b_mod, w_in, b_in, q_gain, k_gain, w_out, b_out):
        n_batch, rows, dim = hidden.shape
        n_item = n_batch // n_shard
        me = lax.axis_index('sp')
        to = lambda rel: [(i, i ^ rel) for i in range(n_shard)]
        by_owner = hidden.reshape(n_shard, n_item, rows, dim)

        def share(rel):
            return lax.dynamic_slice_in_dim(by_owner, me ^ rel, 1, axis=0)

        got = [share(0)] + [lax.ppermute(share(rel), 'sp', to(rel)) for rel in range(1, n_shard)]

        me_arr = me.astype(jnp.int32).reshape(1)
        mod_share = modulation(cond_vec, w_mod, b_mod[:, None, :], me_arr, n_shard)
        mod_all = lax.all_gather(mod_share, 'sp', axis=2, tiled=True)
        mod_mine = lax.dynamic_slice_in_dim(mod_all, me * n_item, n_item, axis=1).astype(jnp.float32)[:, :, None, :]
        pos_all = lax.all_gather(pos_ids, 'sp', axis=0, tiled=False)
        cos, sin = rope_tables(pos_all[me ^ jnp.arange(n_shard)])
        gains = jnp.stack([q_gain, k_gain], axis=1).astype(jnp.float32)[:, :, None, :]
        b_in3 = b_in[:, None, :]
        b_out3 = b_out[:, None, :]
        zero = jnp.zeros((1,), jnp.int32)
        half = n_shard // 2

        near = jnp.concatenate(got[:half], axis=0)
        far = jnp.concatenate(got[half:], axis=0)
        h = proj_in(near, mod_mine[0], w_in, b_in3, gains[0], cos, sin, 0, n_shard)
        h = proj_in(far, mod_mine[0], w_in, b_in3, gains[0], cos, sin, 0, n_shard, first=half, prev=h)
        o = attention(h, dim)
        x = proj_out(o, h, w_out, b_out3, near, mod_mine[0], 0, zero, n_shard, count=half)
        x = proj_out(o, h, w_out, b_out3, far, mod_mine[0], 0, zero + half, n_shard, first=half, count=half, prev=x)

        h = proj_in(x, mod_mine[1], w_in, b_in3, gains[1], cos, sin, 1, n_shard)
        o = attention(h, dim)
        sent = {}
        for rel in (2, 3, 1):
            y = proj_out(o, h, w_out, b_out3, x, mod_mine[1], 1, zero, 1, first=rel, x_first=rel, count=1)
            sent[rel] = lax.ppermute(y, 'sp', to(rel))
        out = proj_out(o, h, w_out, b_out3, x, mod_mine[1], 1, me_arr, n_shard, first=0, x_first=0, count=1)
        for rel in (1, 2, 3):
            out = lax.dynamic_update_slice_in_dim(out, sent[rel], me ^ rel, axis=0)
        return out.reshape(n_batch, rows, dim)

    in_specs = (row_spec, P('dp', None), P('sp', None)) + (P(),) * 8
    return jax.shard_map(local_forward, mesh=mesh, in_specs=in_specs, out_specs=row_spec, check_vma=False)
```

```python
import functools
import math
import jax
import jax.numpy as jnp
from jax import lax
from jax.experimental import pallas as pl
from jax.experimental.pallas import tpu as pltpu
from jax.sharding import PartitionSpec as P

HEAD = 128
ROPE_SPLIT = (16, 56, 56)
ROPE_THETA = 10000.0
NORM_EPS = 1e-6
MIB = 1024 * 1024
LN_ROWS = 16


def rope_tables(pos):
    parts = []
    for column, rope_dim in enumerate(ROPE_SPLIT):
        inv_freq = 1.0 / (ROPE_THETA ** (jnp.arange(0, rope_dim, 2, dtype=jnp.float32) / rope_dim))
        parts.append(pos[..., column:column + 1].astype(jnp.float32) * jnp.repeat(inv_freq, 2))
    angles = jnp.concatenate(parts, axis=-1)
    sign = jnp.where(jnp.arange(HEAD) % 2 == 0, -1.0, 1.0)
    return jnp.cos(angles), jnp.sin(angles) * sign


def mod_kernel(me_ref, c_ref, w_ref, b_ref, o_ref):
    act = jax.nn.silu(c_ref[...].astype(jnp.float32)).astype(jnp.bfloat16)
    vals = jnp.dot(act, w_ref[0], preferred_element_type=jnp.float32) + b_ref[0].astype(jnp.float32)
    o_ref[0] = vals.astype(jnp.bfloat16)


def modulation(cond_vec, w_mod, b_mod, me, n_shard):
    n_layer, dim, width = w_mod.shape
    n_item = cond_vec.shape[0]
    share = width // n_shard
    cols = share // 2
    return pl.pallas_call(
        mod_kernel,
        grid_spec=pltpu.PrefetchScalarGridSpec(
            num_scalar_prefetch=1,
            grid=(n_layer, 2),
            in_specs=[
                pl.BlockSpec((n_item, dim), lambda l, j, me: (0, 0)),
                pl.BlockSpec((1, dim, cols), lambda l, j, me: (l, 0, me[0] * 2 + j)),
                pl.BlockSpec((1, 1, cols), lambda l, j, me: (l, 0, me[0] * 2 + j)),
            ],
            out_specs=pl.BlockSpec((1, n_item, cols), lambda l, j, me: (l, 0, j)),
        ),
        out_shape=jax.ShapeDtypeStruct((n_layer, n_item, share), jnp.bfloat16),
        compiler_params=pltpu.CompilerParams(vmem_limit_bytes=48 * MIB),
        name="modulation",
    )(me, cond_vec, w_mod, b_mod)


def proj_in_kernel(x_ref, mod_ref, w_ref, b_ref, gain_ref, cos_ref, sin_ref, *rest, n_qk, n_v, sub, cols):
    out_ref, u_ref, acc_ref = rest[-3:]
    j = pl.program_id(1)
    _, n_item, rows, dim = x_ref.shape
    width = w_ref.shape[2]

    parts = [slice(s * sub, (s + 1) * sub) for s in range(rows // sub)]

    def norm(t, r):
        shift = mod_ref[t, :, :dim]
        scale = 1.0 + mod_ref[t, :, dim:2 * dim]
        for i in range(r.start, r.stop, LN_ROWS):
            x = x_ref[0, t, i:i + LN_ROWS, :].astype(jnp.float32)
            x = x - jnp.mean(x, axis=-1, keepdims=True)
            x = x * lax.rsqrt(jnp.mean(x * x, axis=-1, keepdims=True) + NORM_EPS)
            u_ref[t, i:i + LN_ROWS, :] = (scale * x + shift).astype(jnp.bfloat16)

    work = [(r, c0) for r in parts for c0 in range(0, width, cols)]
    assert len(work) % 2 == 0

    def pieces(finish, with_norm=False):
        if with_norm:
            norm(0, parts[0])

        def step(t, carry):
            waiting = (1, jnp.maximum(t - 1, 0)) + work[-1]
            for i, (r, c0) in enumerate(work):
                acc_ref[i % 2] = jnp.dot(u_ref[t, r, :], w_ref[0, :, c0:c0 + cols], preferred_element_type=jnp.float32)
                finish(*waiting)
                waiting = (i % 2, t, r, c0)
                if with_norm and c0 == 0:
                    p = parts.index(r) + 1
                    if p < len(parts):
                        norm(t, parts[p])
                    else:
                        norm(jnp.minimum(t + 1, n_item - 1), parts[0])
            return carry

        lax.fori_loop(0, n_item, step, 0)
        finish(1, n_item - 1, *work[-1])

    def biased(slot, c0):
        return (acc_ref[slot] + b_ref[0, :, c0:c0 + cols].astype(jnp.float32)).astype(jnp.bfloat16)

    even = lax.broadcasted_iota(jnp.int32, (sub, HEAD), 1) % 2 == 0

    def rotate(gain):
        def finish(slot, t, r, c0):
            h = biased(slot, c0).astype(jnp.float32)
            for d in range(0, cols, HEAD):
                v = h[:, d:d + HEAD]
                v = v * lax.rsqrt(jnp.mean(v * v, axis=-1, keepdims=True) + NORM_EPS) * gain
                swapped = jnp.where(even, pltpu.roll(v, HEAD - 1, 1), pltpu.roll(v, 1, 1))
                out_ref[0, t, r, c0 + d:c0 + d + HEAD] = (v * cos_ref[0, r, :] + swapped * sin_ref[0, r, :]).astype(jnp.bfloat16)

        return finish

    @pl.when(j == 0)
    def _():
        pieces(rotate(gain_ref[0]), with_norm=True)

    @pl.when((j > 0) & (j < 2 * n_qk))
    def _():
        pieces(rotate(jnp.where(j < n_qk, gain_ref[0], gain_ref[1])))

    @pl.when((j >= 2 * n_qk) & (j < 2 * n_qk + n_v))
    def _():
        def finish(slot, t, r, c0):
            out_ref[0, t, r, c0:c0 + cols] = biased(slot, c0)

        pieces(finish)

    @pl.when(j >= 2 * n_qk + n_v)
    def _():
        def finish(slot, t, r, c0):
            h = biased(slot, c0).astype(jnp.float32)
            out_ref[0, t, r, c0:c0 + cols] = jax.nn.gelu(h, approximate=True).astype(jnp.bfloat16)

        pieces(finish)


def proj_in(x, mod, w_in, b_in, gain, cos, sin, layer, n_chunk, first=0, prev=None, block=1536, sub=192, cols=512):
    count, n_item, rows, dim = x.shape
    width = w_in.shape[2]
    in_specs = [
        pl.BlockSpec((1, n_item, rows, dim), lambda r, j: (r, 0, 0, 0)),
        pl.BlockSpec((n_item, 1, 3 * dim), lambda r, j: (0, 0, 0)),
        pl.BlockSpec((1, dim, block), lambda r, j: (layer, 0, j)),
        pl.BlockSpec((1, 1, block), lambda r, j: (layer, 0, j)),
        pl.BlockSpec((2, 1, HEAD), lambda r, j: (0, 0, 0)),
        pl.BlockSpec((1, rows, HEAD), lambda r, j: (first + r, 0, 0)),
        pl.BlockSpec((1, rows, HEAD), lambda r, j: (first + r, 0, 0)),
    ]
    operands = [x, mod, w_in, b_in, gain, cos, sin]
    aliases = {}
    if prev is not None:
        in_specs.append(pl.BlockSpec(memory_space=pl.ANY))
        operands.append(prev)
        aliases = {7: 0}
    return pl.pallas_call(
        functools.partial(proj_in_kernel, n_qk=dim // block, n_v=dim // block, sub=sub, cols=cols),
        grid=(count, width // block),
        in_specs=in_specs,
        out_specs=pl.BlockSpec((1, n_item, rows, block), lambda r, j: (first + r, 0, 0, j)),
        out_shape=jax.ShapeDtypeStruct((n_chunk, n_item, rows, width), jnp.bfloat16),
        scratch_shapes=[pltpu.VMEM((n_item, rows, dim), jnp.bfloat16), pltpu.VMEM((2, sub, cols), jnp.float32)],
        input_output_aliases=aliases,
        compiler_params=pltpu.CompilerParams(vmem_limit_bytes=60 * MIB),
        cost_estimate=pl.CostEstimate(flops=2 * count * n_item * rows * dim * width, bytes_accessed=2 * count * (dim * width + n_item * rows * width), transcendentals=0),
        name="proj_in",
    )(*operands)


def attention_kernel(q_ref, k_ref, v_ref, o_ref, s_ref, *, n_head, sub):
    n_chunk, _, rows, _ = q_ref.shape
    keys = n_chunk * rows
    exp_scale = HEAD ** -0.5 * math.log2(math.e)
    work = [(slice(h * HEAD, (h + 1) * HEAD), c, slice(s * sub, (s + 1) * sub)) for h in range(n_head) for c in range(n_chunk) for s in range(rows // sub)]

    def score(i):
        head, c, r = work[i]
        k = k_ref[:, 0, :, head].reshape(keys, HEAD)
        s_ref[i % 2] = lax.dot_general(q_ref[c, 0, r, head], k, (((1,), (1,)), ((), ())), preferred_element_type=jnp.float32)

    score(0)
    for i, (head, c, r) in enumerate(work):
        if i + 1 < len(work):
            score(i + 1)
        s = s_ref[i % 2]
        p = jnp.exp2((s - jnp.max(s, axis=-1, keepdims=True)) * exp_scale)
        total = jnp.sum(p, axis=-1, keepdims=True)
        v = v_ref[:, 0, :, head].reshape(keys, HEAD)
        o = jnp.dot(p.astype(jnp.bfloat16), v, preferred_element_type=jnp.float32)
        o_ref[c, 0, r, head] = (o / total).astype(jnp.bfloat16)


def attention(h, dim, n_head=4, sub=384):
    n_chunk, n_item, rows, _ = h.shape
    w = n_head * HEAD
    nb = dim // w
    block = (n_chunk, 1, rows, w)
    keys = n_chunk * rows
    return pl.pallas_call(
        functools.partial(attention_kernel, n_head=n_head, sub=sub),
        grid=(n_item, nb),
        in_specs=[
            pl.BlockSpec(block, lambda t, g: (0, t, 0, g)),
            pl.BlockSpec(block, lambda t, g: (0, t, 0, nb + g)),
            pl.BlockSpec(block, lambda t, g: (0, t, 0, 2 * nb + g)),
        ],
        out_specs=pl.BlockSpec(block, lambda t, g: (0, t, 0, g)),
        out_shape=jax.ShapeDtypeStruct((n_chunk, n_item, rows, dim), jnp.bfloat16),
        scratch_shapes=[pltpu.VMEM((2, sub, keys), jnp.float32)],
        compiler_params=pltpu.CompilerParams(vmem_limit_bytes=60 * MIB),
        cost_estimate=pl.CostEstimate(flops=4 * n_item * keys * keys * dim, bytes_accessed=8 * n_item * keys * dim, transcendentals=n_item * keys * keys * dim // HEAD),
        name="attention",
    )(h, h, h)


def proj_out_kernel(slot_ref, o_ref, g_ref, w_ref, b_ref, x_ref, mod_ref, *rest, k_attn, sub, cols):
    out_ref, acc_ref = rest[-2:]
    k = pl.program_id(1)
    last = pl.num_programs(1) - 1
    n_item, rows, dim = acc_ref.shape
    tiles = [(slice(s * sub, (s + 1) * sub), slice(n * cols, (n + 1) * cols)) for s in range(rows // sub) for n in range(dim // cols)]

    def each_tile(fn):
        def step(t, carry):
            for r, c in tiles:
                fn(t, r, c)
            return carry

        lax.fori_loop(0, n_item, step, 0)

    def product(src, t, r, c):
        return jnp.dot(src[0, t, r, :], w_ref[0, :, c], preferred_element_type=jnp.float32)

    @pl.when(k == 0)
    def _():
        def fn(t, r, c):
            acc_ref[t, r, c] = product(o_ref, t, r, c)

        each_tile(fn)

    @pl.when((k > 0) & (k < k_attn))
    def _():
        def fn(t, r, c):
            acc_ref[t, r, c] += product(o_ref, t, r, c)

        each_tile(fn)

    @pl.when((k >= k_attn) & (k < last))
    def _():
        def fn(t, r, c):
            acc_ref[t, r, c] += product(g_ref, t, r, c)

        each_tile(fn)

    @pl.when(k == last)
    def _():
        def fn(t, r, c):
            y = acc_ref[t, r, c] + product(g_ref, t, r, c) + b_ref[0, :, c].astype(jnp.float32)
            gate = mod_ref[t, :, 2 * dim + c.start:2 * dim + c.stop]
            y = gate * y.astype(jnp.bfloat16).astype(jnp.float32)
            out_ref[0, t, r, c] = (x_ref[0, t, r, c].astype(jnp.float32) + y).astype(jnp.bfloat16)

        each_tile(fn)


def proj_out(o, h, w_out, b_out, x, mod, layer, slot, out_slots, first=0, x_first=0, count=None, prev=None, k_block=1536, sub=384, cols=512):
    _, n_item, rows, dim = o.shape
    depth = w_out.shape[1]
    k_attn = dim // k_block
    g_off = 3 * dim // k_block - k_attn
    in_specs = [
        pl.BlockSpec((1, n_item, rows, k_block), lambda r, k, sl: (first + r, 0, 0, jnp.minimum(k, k_attn - 1))),
        pl.BlockSpec((1, n_item, rows, k_block), lambda r, k, sl: (first + r, 0, 0, g_off + jnp.maximum(k, k_attn))),
        pl.BlockSpec((1, k_block, dim), lambda r, k, sl: (layer, k, 0)),
        pl.BlockSpec((1, 1, dim), lambda r, k, sl: (layer, 0, 0)),
        pl.BlockSpec((1, n_item, rows, dim), lambda r, k, sl: (x_first + r, 0, 0, 0)),
        pl.BlockSpec((n_item, 1, 3 * dim), lambda r, k, sl: (0, 0, 0)),
    ]
    operands = [slot, o, h, w_out, b_out, x, mod]
    aliases = {}
    if prev is not None:
        in_specs.append(pl.BlockSpec(memory_space=pl.ANY))
        operands.append(prev)
        aliases = {7: 0}
    return pl.pallas_call(
        functools.partial(proj_out_kernel, k_attn=k_attn, sub=sub, cols=cols),
        grid_spec=pltpu.PrefetchScalarGridSpec(
            num_scalar_prefetch=1,
            grid=(count, depth // k_block),
            in_specs=in_specs,
            out_specs=pl.BlockSpec((1, n_item, rows, dim), lambda r, k, sl: (sl[0] + r, 0, 0, 0)),
            scratch_shapes=[pltpu.VMEM((n_item, rows, dim), jnp.float32)],
        ),
        out_shape=jax.ShapeDtypeStruct((out_slots, n_item, rows, dim), jnp.bfloat16),
        input_output_aliases=aliases,
        compiler_params=pltpu.CompilerParams(vmem_limit_bytes=62 * MIB),
        cost_estimate=pl.CostEstimate(flops=2 * count * n_item * rows * dim * depth, bytes_accessed=2 * count * dim * depth, transcendentals=0),
        name="proj_out",
    )(*operands)


def solution(mesh):
    row_spec = P('dp', 'sp', None)
    n_shard = mesh.shape['sp']

    def local_forward(hidden, cond_vec, pos_ids, w_mod, b_mod, w_in, b_in, q_gain, k_gain, w_out, b_out):
        n_batch, rows, dim = hidden.shape
        n_item = n_batch // n_shard
        me = lax.axis_index('sp')
        to = lambda rel: [(i, i ^ rel) for i in range(n_shard)]
        me_arr = me.astype(jnp.int32).reshape(1)
        mod_share = modulation(cond_vec, w_mod, b_mod[:, None, :], me_arr, n_shard)
        mod_all = lax.all_gather(mod_share, 'sp', axis=2, tiled=True)
        pos_all = lax.all_gather(pos_ids, 'sp', axis=0, tiled=False)
        by_owner, mod_all, pos_all = lax.optimization_barrier((hidden.reshape(n_shard, n_item, rows, dim), mod_all, pos_all))

        def share(rel):
            return lax.dynamic_slice_in_dim(by_owner, me ^ rel, 1, axis=0)

        got = [share(0)] + [lax.ppermute(share(rel), 'sp', to(rel)) for rel in range(1, n_shard)]
        mod_mine = lax.dynamic_slice_in_dim(mod_all, me * n_item, n_item, axis=1).astype(jnp.float32)[:, :, None, :]
        cos, sin = rope_tables(pos_all[me ^ jnp.arange(n_shard)])
        gains = jnp.stack([q_gain, k_gain], axis=1).astype(jnp.float32)[:, :, None, :]
        b_in3 = b_in[:, None, :]
        b_out3 = b_out[:, None, :]
        zero = jnp.zeros((1,), jnp.int32)
        half = n_shard // 2

        near = jnp.concatenate(got[:half], axis=0)
        far = jnp.concatenate(got[half:], axis=0)
        h = proj_in(near, mod_mine[0], w_in, b_in3, gains[0], cos, sin, 0, n_shard)
        h = proj_in(far, mod_mine[0], w_in, b_in3, gains[0], cos, sin, 0, n_shard, first=half, prev=h)
        o = attention(h, dim)
        x = proj_out(o, h, w_out, b_out3, near, mod_mine[0], 0, zero, n_shard, count=half)
        x = proj_out(o, h, w_out, b_out3, far, mod_mine[0], 0, zero + half, n_shard, first=half, count=half, prev=x)

        h = proj_in(x, mod_mine[1], w_in, b_in3, gains[1], cos, sin, 1, n_shard)
        o = attention(h, dim)
        sent = {}
        for rel in (2, 3, 1):
            y = proj_out(o, h, w_out, b_out3, x, mod_mine[1], 1, zero, 1, first=rel, x_first=rel, count=1)
            sent[rel] = lax.ppermute(y, 'sp', to(rel))
        out = proj_out(o, h, w_out, b_out3, x, mod_mine[1], 1, me_arr, n_shard, first=0, x_first=0, count=1)
        for rel in (1, 2, 3):
            out = lax.dynamic_update_slice_in_dim(out, sent[rel], me ^ rel, axis=0)
        return out.reshape(n_batch, rows, dim)

    in_specs = (row_spec, P('dp', None), P('sp', None)) + (P(),) * 8
    return jax.shard_map(local_forward, mesh=mesh, in_specs=in_specs, out_specs=row_spec, check_vma=False)
```
